128 devices in a mesh: groups: 4 (over x, y), blk: 32 (over z, core).
Axes of the slice: x: 2, y: 2, z: 16, core: 2. Of those that a mesh axis runs over, the one named last changes fastest.
The devices are a block of a 8x8x16 slice.
Arguments:
- points: bfloat16 [196608, 1024], P(('groups', 'blk')), parts along dimension 0, may hold values from -6 to 6
- coverage: float32 [196608], P(('groups', 'blk')), parts along dimension 0, may hold values from 0 to 1.5
- candidates: bfloat16 [16384, 1024], P(('groups', 'blk')), parts along dimension 0, may hold values from -6 to 6
- cand_count: int32 [128], P(('groups', 'blk')), parts along dimension 0, may hold values from 16 to 128, as said below
- acc_index: int32 [128, 16], P(('groups', 'blk')), parts along dimension 0, may hold values from 0 to 127, as said below
Outputs:
- gain_out: float32 [16384], P(('groups', 'blk')), parts along dimension 0
- new_coverage: float32 [196608], P(('groups', 'blk')), parts along dimension 0
The draws below stay inside these ranges and needn't reach their ends.
There are 4 independent parts, one for each index of `groups`. The reference program is written for one: setup_inputs(seed, part) draws one part's arguments, and reference() takes and returns one part's arrays. A program takes and returns all parts, laid end to end along the dimension named above; each array names one. Nothing has to cross between parts.
Inputs may be any that keep to these rules, and one draw needn't show every extreme that they name: `cand_count`: some device has all 128 slots live. `acc_index`: each entry of row b is below cand_count[b]; entries may repeat.
All inputs are finite; a program needn't handle non-finite values.
Results may differ from the reference program's by a relative error of at most 0.0003.
Values may be sent and summed in bfloat16 or wider, within the bound.
A program may use at most 64 MiB of HBM per device.

```python
import jax
import jax.numpy as jnp
from jax import lax

D = 1024
CAND_DEV = 128
ACC_DEV = 16
PTS = 49152
CANDS = 4096
N_BLK = 32


def shared_counts(key):
    first, second = jax.random.split(jax.random.fold_in(key, 7))
    counts = jax.random.randint(first, (N_BLK,), ACC_DEV, CAND_DEV + 1)
    chosen = jax.random.randint(second, (), 0, N_BLK)
    return jnp.where(jnp.arange(N_BLK) == chosen, CAND_DEV, counts).astype(jnp.int32)


def draw_cand_count(key, part):
    return shared_counts(key)


def draw_acc_index(key, part):
    counts = shared_counts(key)
    picked = jax.random.randint(jax.random.fold_in(key, 11), (N_BLK, ACC_DEV), 0, counts[:, None])
    return picked.astype(jnp.int32)


def levels(stream_key, dims, cuts, least, high):
    def one(axis_at, parts):
        heights = jax.random.uniform(jax.random.fold_in(jax.random.fold_in(stream_key, 6), axis_at), (parts,), jnp.float32, least / len(cuts), high / len(cuts))
        return jnp.repeat(jnp.exp(heights), dims[axis_at] // parts).reshape((-1,) + (1,) * (len(dims) - axis_at - 1))

    loudness = one(*cuts[0])
    for cut in cuts[1:]:
        loudness = loudness * one(*cut)
    return loudness


def noise(key, dims, width, bound, cuts=(), kind=jnp.bfloat16):
    result = jax.random.normal(key, dims, jnp.float32) * width
    if len(cuts) > 0:
        result = levels(key, dims, cuts, -0.22, 0.18) * result
    return jnp.clip(result, min=-bound, max=bound).astype(kind)


def setup_inputs(seed: int = 0, part: int = 0) -> dict:
    arg_keys = jax.random.split(jax.random.key(seed), 6)
    part_splits = jax.random.split(jax.random.fold_in(arg_keys[5], part), 6)
    points = noise(part_splits[0], (PTS, D), 1.0, 6.0, ((0, 32),))
    coverage = jnp.clip(1.5 * jax.random.uniform(part_splits[1], (PTS,), jnp.float32) ** levels(part_splits[1], (PTS,), ((0, 32),), -0.2, 0.2), 0.0, 1.5)
    candidates = noise(part_splits[2], (CANDS, D), 1.0, 6.0, ((0, 32),))
    cand_count = draw_cand_count(jax.random.fold_in(jax.random.fold_in(arg_keys[5], part), 71), part)
    acc_index = draw_acc_index(jax.random.fold_in(jax.random.fold_in(arg_keys[5], part), 71), part)
    return dict(points=points, coverage=coverage, candidates=candidates, cand_count=cand_count, acc_index=acc_index)


def block_gains(points, coverage, cand_block, factor):
    similar = jnp.dot(points, cand_block.T, preferred_element_type=jnp.float32) * factor
    return lax.optimization_barrier(jnp.sum(jnp.maximum(similar - coverage[:, None], 0.0), axis=0))

def reference(points, coverage, candidates, cand_count, acc_index):
    factor = 1.0 / jnp.sqrt(jnp.float32(D))
    blocks = candidates.reshape(N_BLK, CAND_DEV, D)
    gain_sum = lax.map(lambda cand_block: block_gains(points, coverage, cand_block, factor), blocks)
    live_rows = jnp.arange(CAND_DEV, dtype=jnp.int32)[None, :] < cand_count[:, None]
    gain_out = jnp.where(live_rows, gain_sum / jnp.float32(PTS), 0.0).reshape(CANDS)
    rows_taken = (jnp.arange(N_BLK, dtype=jnp.int32)[:, None] * CAND_DEV + acc_index).reshape(-1)
    accepted = jnp.take(candidates, rows_taken, axis=0)
    similar = jnp.dot(points, accepted.T, preferred_element_type=jnp.float32) * factor
    new_coverage = jnp.maximum(coverage, lax.optimization_barrier(jnp.max(similar, axis=1)))
    return (gain_out, new_coverage)
```

```python
import functools

import jax
import jax.numpy as jnp
from jax import lax
from jax.experimental import pallas as pl
from jax.experimental.pallas import tpu as pltpu
from jax.sharding import PartitionSpec as P

GROUPS_BLK = ("groups", "blk")
CORES = 2
LANES = 128
CHUNK = 32
TILE = 256
DEAD = -3.0e38


def kernel(
    chips, total_points, count_ref, acc_ref, points_hbm, cover_ref, cands_hbm,
    gain_ref, newcov_ref,
    pts, rows, covb, best, marks, gacc, sums, inbox,
    load_sem, send_sem, recv_sem, push_sem, land_sem, mark_send, mark_recv, mark_push, mark_land,
    sum_send, sum_recv,
):
    npts, width = pts.shape
    slots = cands_hbm.shape[0]
    chip_rows = CORES * slots
    per_block = slots // CHUNK
    half = per_block // 2
    far = chips // 2
    steps = (far - 1) * per_block + half
    tiles = npts // TILE
    scale = jnp.sqrt(jnp.float32(width))
    factor = 1.0 / scale

    me = lax.axis_index("blk")
    z, core = me // CORES, me % CORES
    up = ((z + 1) % chips) * CORES + core
    down = ((z + chips - 1) % chips) * CORES + core
    partner = z * CORES + (1 - core)

    own = pltpu.make_async_copy(
        cands_hbm, rows.at[pl.ds(pl.multiple_of(core * slots, slots), slots)], load_sem.at[0]
    )
    own.start()
    resident = pltpu.make_async_copy(points_hbm, pts, load_sem.at[1])
    resident.start()

    lane = lax.broadcasted_iota(jnp.int32, (1, LANES), 1)
    mark = jnp.full((1, LANES), DEAD, jnp.float32)
    for a in range(acc_ref.shape[1]):
        mark = jnp.where(lane == acc_ref[0, a], 0.0, mark)
    marks[core] = mark

    barrier = pltpu.get_barrier_semaphore()
    for neighbour in (up, down, partner):
        pl.semaphore_signal(barrier, inc=1, device_id={"blk": neighbour})
    pl.semaphore_wait(barrier, 3)

    def slot_of(way, hop):
        return hop if way == 0 else (chips - hop) % chips

    def chunk_rows(way, hop, j, c):
        if way == 1:
            j = (j + half) % per_block
        start = slot_of(way, hop) * chip_rows + c * slots + j * CHUNK
        return pl.ds(pl.multiple_of(start, CHUNK), CHUNK)

    def send(way, k):
        hop, j = k // per_block, k % per_block
        return pltpu.make_async_remote_copy(
            src_ref=rows.at[chunk_rows(way, hop, j, core)],
            dst_ref=rows.at[chunk_rows(way, hop + 1, j, core)],
            send_sem=send_sem.at[way, k],
            recv_sem=recv_sem.at[way, k],
            device_id={"blk": up if way == 0 else down},
        )

    def push(way, k):
        hop, j = k // per_block, k % per_block
        at = rows.at[chunk_rows(way, hop + 1, j, core)]
        return pltpu.make_async_remote_copy(
            src_ref=at, dst_ref=at, send_sem=push_sem.at[way, k], recv_sem=land_sem.at[way, k],
            device_id={"blk": partner},
        )

    def mark_send_of(way, hop):
        return pltpu.make_async_remote_copy(
            src_ref=marks.at[slot_of(way, hop) * CORES + core],
            dst_ref=marks.at[slot_of(way, hop + 1) * CORES + core],
            send_sem=mark_send.at[way, hop],
            recv_sem=mark_recv.at[way, hop],
            device_id={"blk": up if way == 0 else down},
        )

    def mark_push_of(way, hop):
        at = marks.at[slot_of(way, hop) * CORES + core]
        return pltpu.make_async_remote_copy(
            src_ref=at, dst_ref=at, send_sem=mark_push.at[way, hop], recv_sem=mark_land.at[way, hop],
            device_id={"blk": partner},
        )

    own_at = rows.at[pl.ds(pl.multiple_of(core * slots, slots), slots)]
    own_push = pltpu.make_async_remote_copy(
        src_ref=own_at, dst_ref=own_at, send_sem=load_sem.at[2], recv_sem=load_sem.at[3],
        device_id={"blk": partner},
    )

    own.wait()
    for way in (0, 1):
        mark_send_of(way, 0).start()
    for k in range(per_block):
        for way in (0, 1):
            send(way, k).start()
    own_push.start()
    mark_push_of(0, 0).start()

    for t in range(npts // LANES):
        row = cover_ref[pl.ds(t, 1), :] * scale
        col = jnp.broadcast_to(row, (LANES, LANES)).T
        covb[pl.ds(t * LANES, LANES), :] = col
        best[pl.ds(t * LANES, LANES), :] = col
    resident.wait()

    def tile_work(slot, tile):
        at = pl.ds(pl.multiple_of(tile * TILE, TILE), TILE)
        block = rows[pl.ds(pl.multiple_of(slot * chip_rows, chip_rows), chip_rows), :]
        similar = lax.dot_general(
            pts[at, :], block, (((1,), (1,)), ((), ())), preferred_element_type=jnp.float32
        )
        cover = covb[at, :]
        high = best[at, :]
        for c in range(CORES):
            mine = similar[:, c * slots : (c + 1) * slots]
            over = jnp.maximum(mine - cover, 0.0)
            gacc[c] += jnp.sum(over.reshape(TILE // 8, 8, slots), axis=0)
            high = jnp.maximum(high, mine + marks[slot * CORES + c])
        best[at, :] = high

    def clear():
        gacc[...] = jnp.zeros_like(gacc)

    def store_sums(slot):
        for c in range(CORES):
            sums[slot * CORES + c] = jnp.sum(gacc[c], axis=0, keepdims=True)

    def sum_copy(slot, owner_core):
        owner = ((z + chips - slot) % chips) * CORES + owner_core
        return pltpu.make_async_remote_copy(
            src_ref=sums.at[slot * CORES + owner_core],
            dst_ref=inbox.at[slot * CORES + (core + owner_core) % CORES],
            send_sem=sum_send,
            recv_sem=sum_recv,
            device_id={"blk": owner},
        )

    def send_sums(slot):
        for c in range(CORES):
            sum_copy(slot, c).start()

    def run_tiles(slot, first, last):
        def body(tile, carry):
            tile_work(slot, tile)
            return carry

        lax.fori_loop(first, last, body, 0)

    def arrive(k, forward):
        for way in (0, 1):
            send(way, k).wait_recv()
            if forward is True:
                send(way, k + per_block).start()
            elif forward is not None:

                @pl.when(forward)
                def _():
                    send(way, k + per_block).start()

            push(way, k).start()

    def mark_arrive(hop, ways, forward_ways):
        for way in ways:
            mark_send_of(way, hop - 1).wait_recv()
            if way in forward_ways:
                mark_send_of(way, hop).start()
            mark_push_of(way, hop).start()

    def landed(hop, ways):
        for way in ways:
            for j in range(per_block):
                push(way, (hop - 1) * per_block + j).wait_recv()
            mark_push_of(way, hop).wait_recv()

    mark_arrive(1, (0, 1), (0, 1))
    own_push.wait_recv()
    mark_push_of(0, 0).wait_recv()
    clear()
    for j in range(per_block):
        run_tiles(0, j * tiles // per_block, (j + 1) * tiles // per_block)
        arrive(j, True)
    store_sums(0)

    def hop_body(hop, carry):
        for way in (0, 1):
            mark_send_of(way, hop).wait_recv()
            if way == 0:
                mark_send_of(way, hop + 1).start()
            else:

                @pl.when(hop < far - 2)
                def _():
                    mark_send_of(1, hop + 1).start()

            mark_push_of(way, hop + 1).start()
        for j in range(per_block):
            k = hop * per_block + j
            arrive(k, True if j < half else hop < far - 2)
            if j % half == 0:
                way = j // half
                landed(hop, (way,))
                clear()
            slot = slot_of(j // half, hop)
            run_tiles(slot, (j % half) * tiles // half, (j % half + 1) * tiles // half)
            if j % half == half - 1:
                store_sums(slot)
                send_sums(slot)
        return carry

    lax.fori_loop(1, far - 1, hop_body, 0)

    mark_arrive(far, (0,), ())
    for way in (0, 1):
        for j in range(way * half, way * half + half):
            if j % half == 0:
                landed(far - 1, (way,))
                clear()
            if way == 0:
                arrive((far - 1) * per_block + j, None)
            slot = slot_of(way, far - 1)
            run_tiles(slot, (j % half) * tiles // half, (j % half + 1) * tiles // half)
        store_sums(slot)
        send_sums(slot)
    for way in (0, 1):
        for j in range(half):
            push(way, (far - 1) * per_block + j).wait_recv()
    mark_push_of(0, far).wait_recv()
    clear()
    run_tiles(far, 0, tiles)
    store_sums(far)
    send_sums(far)

    sum_copy(0, 1 - core).start()
    inbox[0] = sums[core]

    for t in range(npts // LANES):
        newcov_ref[pl.ds(t, 1), :] = (
            jnp.max(best[pl.ds(t * LANES, LANES), :].T, axis=0, keepdims=True) * factor
        )

    own_push.wait_send()
    for way in (0, 1):
        for k in range(steps):
            send(way, k).wait_send()
            push(way, k).wait_send()
        for hop in range(far if way == 0 else far - 1):
            mark_send_of(way, hop).wait_send()
            mark_push_of(way, hop + 1).wait_send()
    mark_push_of(0, 0).wait_send()

    others = chips * CORES - 1
    pltpu.make_async_copy(sums.at[pl.ds(0, others)], sums.at[pl.ds(0, others)], sum_send).wait()
    pltpu.make_async_copy(inbox.at[pl.ds(1, others)], inbox.at[pl.ds(1, others)], sum_recv).wait()
    total = jnp.sum(inbox[...], axis=0)
    gain_ref[...] = jnp.where(lane < count_ref[0], total * factor / total_points, 0.0)


def per_device(points, coverage, candidates, cand_count, acc_index):
    npts, width = points.shape
    slots = candidates.shape[0]
    blocks = lax.axis_size("blk")
    chips = blocks // CORES
    per_block = slots // CHUNK
    steps = (chips // 2 - 1) * per_block + per_block // 2
    vmem = pl.BlockSpec(memory_space=pltpu.VMEM)
    smem = pl.BlockSpec(memory_space=pltpu.SMEM)
    hbm = pl.BlockSpec(memory_space=pl.ANY)
    dma = pltpu.SemaphoreType.DMA
    gain, cover = pl.pallas_call(
        functools.partial(kernel, chips, float(npts * blocks)),
        out_shape=(
            jax.ShapeDtypeStruct((1, slots), jnp.float32),
            jax.ShapeDtypeStruct((npts // LANES, LANES), jnp.float32),
        ),
        in_specs=[smem, smem, hbm, vmem, hbm],
        out_specs=(vmem, vmem),
        scratch_shapes=[
            pltpu.VMEM((npts, width), jnp.bfloat16),
            pltpu.VMEM((blocks * slots, width), jnp.bfloat16),
            pltpu.VMEM((npts, LANES), jnp.float32),
            pltpu.VMEM((npts, LANES), jnp.float32),
            pltpu.VMEM((blocks, 1, slots), jnp.float32),
            pltpu.VMEM((CORES, 8, slots), jnp.float32),
            pltpu.VMEM((blocks, 1, slots), jnp.float32),
            pltpu.VMEM((blocks, 1, slots), jnp.float32),
            dma((4,)),
            dma((2, steps)),
            dma((2, steps)),
            dma((2, steps)),
            dma((2, steps)),
            dma((2, chips // 2 + 1)),
            dma((2, chips // 2 + 1)),
            dma((2, chips // 2 + 1)),
            dma((2, chips // 2 + 1)),
            dma,
            dma,
        ],
        compiler_params=pltpu.CompilerParams(
            collective_id=0, has_side_effects=True, vmem_limit_bytes=48 * 1024 * 1024
        ),
        cost_estimate=pl.CostEstimate(
            flops=2 * npts * width * blocks * slots, bytes_accessed=npts * width * 2, transcendentals=0
        ),
    )(cand_count, acc_index, points, coverage.reshape(npts // LANES, LANES), candidates)
    return gain.reshape(slots), cover.reshape(npts)


def solution(mesh):
    return jax.shard_map(
        per_device,
        mesh=mesh,
        in_specs=(
            P(GROUPS_BLK, None),
            P(GROUPS_BLK),
            P(GROUPS_BLK, None),
            P(GROUPS_BLK),
            P(GROUPS_BLK, None),
        ),
        out_specs=(P(GROUPS_BLK), P(GROUPS_BLK)),
        check_vma=False,
    )
```

```python
import functools

import jax
import jax.numpy as jnp
from jax import lax
from jax.experimental import pallas as pl
from jax.experimental.pallas import tpu as pltpu
from jax.sharding import PartitionSpec as P

GROUPS_BLK = ("groups", "blk")
CORES = 2
LANES = 128
TILE = 768
SHORT = 2
DEAD = -3.0e38


def kernel(
    chips, total_points, acc_hbm, points_hbm, cover_hbm, cands_hbm,
    gain_ref, newcov_ref,
    acc_ref, cover_ref, pts, rows, covb, best, marks, gacc, sums, inbox, ghost,
    load_sem, send_sem, push_sem, recv_sem, land_sem, sum_sem,
):
    npts, width = pts.shape
    slots = cands_hbm.shape[0]
    chip_rows = CORES * slots
    set_rows = slots // 2
    chunk = set_rows // 2
    short = (chips - 1) // 3
    long = 2 * short
    tiles = npts // TILE
    scale = jnp.sqrt(jnp.float32(width))
    factor = 1.0 / scale

    me = lax.axis_index("blk")
    z, core = me // CORES, me % CORES
    ahead = [((z + 1) % chips) * CORES + core, ((z + chips - 1) % chips) * CORES + core]
    partner = z * CORES + (1 - core)
    lane = lax.broadcasted_iota(jnp.int32, (1, LANES), 1)
    low = lane < set_rows

    own_at = rows.at[pl.ds(pl.multiple_of(core * slots, slots), slots)]
    accepted = pltpu.make_async_copy(acc_hbm, acc_ref, load_sem.at[0])
    own = pltpu.make_async_copy(cands_hbm, own_at, load_sem.at[1])
    covered = pltpu.make_async_copy(cover_hbm, cover_ref, load_sem.at[2])
    resident = pltpu.make_async_copy(points_hbm, pts, load_sem.at[3])
    for load in (accepted, own, covered, resident):
        load.start()

    barrier = pltpu.get_barrier_semaphore()
    for neighbour in (*ahead, partner):
        pl.semaphore_signal(barrier, inc=1, device_id={"blk": neighbour})

    accepted.wait()
    mark = jnp.full((1, LANES), DEAD, jnp.float32)
    for a in range(acc_ref.shape[1]):
        mark = jnp.where(lane == acc_ref[0, a], 0.0, mark)
    for way in (0, 1):
        marks[way * (long + 1) * CORES + core] = mark

    pl.semaphore_wait(barrier, 3)

    def slot_of(way, hop):
        return hop if way == 0 else (chips - hop) % chips

    def rows_at(way, hop, which, part, c):
        start = slot_of(way, hop) * chip_rows + c * slots + which * set_rows + part * chunk
        return rows.at[pl.ds(pl.multiple_of(start, chunk), chunk)]

    def mark_at(way, hop, c):
        return marks.at[(way * (long + 1) + hop) * CORES + c]

    def remote(src, dst, send, recv, device):
        return pltpu.make_async_remote_copy(
            src_ref=src, dst_ref=dst, send_sem=send, recv_sem=recv, device_id={"blk": device}
        )

    def where_of(way, turn, step):
        if step is SHORT:
            return turn // 2 + 1, 1 - way, turn % 2
        return turn + 1, way, step

    def send(way, turn, step):
        hop, which, part = where_of(way, turn, step)
        return remote(
            rows_at(way, hop - 1, which, part, core), rows_at(way, hop, which, part, core),
            send_sem.at[0], recv_sem.at[way, turn, step], ahead[way],
        )

    def send_mark(way, turn):
        return remote(
            mark_at(way, turn, core), mark_at(way, turn + 1, core),
            send_sem.at[1], recv_sem.at[way, turn, 0], ahead[way],
        )

    def landing(turn, step):
        return land_sem.at[long + turn // 2] if step is SHORT else land_sem.at[turn]

    def push(way, turn, step):
        hop, which, part = where_of(way, turn, step)
        at = rows_at(way, hop, which, part, core)
        return remote(at, at, push_sem.at[0], landing(turn, step), partner)

    def push_mark(way, turn):
        at = mark_at(way, turn + 1, core)
        return remote(at, at, push_sem.at[1], landing(turn, 0), partner)

    def wait_bytes(sem, count, ref=None):
        part = (ghost if ref is None else ref).at[pl.ds(0, count)]
        pltpu.make_async_copy(part, part, sem).wait()

    line = rows.shape[1] * 2 // (LANES * 4)
    own_push = [
        remote(own_at, own_at, push_sem.at[0], load_sem.at[4], partner),
        remote(mark_at(0, 0, core), mark_at(0, 0, core), push_sem.at[1], load_sem.at[4], partner),
        remote(mark_at(1, 0, core), mark_at(1, 0, core), push_sem.at[1], load_sem.at[4], partner),
    ]

    for way in (0, 1):
        send_mark(way, 0).start()
    own.wait()
    for step in (0, 1, SHORT):
        for way in (0, 1):
            send(way, 0, step).start()
    for copy in own_push:
        copy.start()

    covered.wait()
    for t in range(npts // LANES):
        row = cover_ref[pl.ds(t, 1), :] * scale
        col = jnp.broadcast_to(row, (LANES, LANES)).T
        covb[pl.ds(t * LANES, LANES), :] = col
        best[pl.ds(t * LANES, LANES), :] = col
    resident.wait()
    wait_bytes(load_sem.at[4], slots * line + 2)

    def tile_work(way, hop, tile):
        at = pl.ds(pl.multiple_of(tile * TILE, TILE), TILE)
        pieces = []
        for c in range(CORES):
            for which, path in ((0, way), (1, 1 - way)):
                start = slot_of(path, hop) * chip_rows + c * slots + which * set_rows
                pieces.append(rows[pl.ds(pl.multiple_of(start, set_rows), set_rows), :])
        similar = lax.dot_general(
            pts[at, :], jnp.concatenate(pieces, axis=0), (((1,), (1,)), ((), ())),
            preferred_element_type=jnp.float32,
        )
        cover = covb[at, :]
        high = best[at, :]
        for c in range(CORES):
            bias = jnp.where(low, mark_at(way, hop, c)[...], mark_at(1 - way, hop, c)[...])
            mine = similar[:, c * slots : (c + 1) * slots]
            over = jnp.maximum(mine - cover, 0.0)
            gacc[c] += jnp.sum(over.reshape(TILE // 8, 8, slots), axis=0)
            high = jnp.maximum(high, mine + bias)
        best[at, :] = high

    def clear():
        gacc[...] = jnp.zeros_like(gacc)

    def store_sums(way, hop):
        for c in range(CORES):
            value = jnp.sum(gacc[c], axis=0, keepdims=True)
            first = slot_of(way, hop) * CORES + c
            second = slot_of(1 - way, hop) * CORES + c
            sums[first] = jnp.where(low, value, sums[first])
            sums[second] = jnp.where(low, sums[second], value)

    def sum_copy(slot, owner_core):
        owner = ((z + chips - slot) % chips) * CORES + owner_core
        return remote(
            sums.at[slot * CORES + owner_core], inbox.at[slot * CORES + (core + owner_core) % CORES],
            sum_sem.at[0], sum_sem.at[1], owner,
        )

    def send_sums(slot):
        for c in range(CORES):
            sum_copy(slot, c).start()

    def round_body(turn, carry):
        @pl.when(turn > 0)
        def _():
            wait_bytes(land_sem.at[turn - 1], 2 * (set_rows * line + 1))

        clear()

        def half_body(step, carry):
            @pl.when(turn < long)
            def _():
                for way in (0, 1):

                    @pl.when(step == 0)
                    def _():
                        wait_bytes(recv_sem.at[way, turn, 0], chunk * line + 1)

                    @pl.when(step != 0)
                    def _():
                        wait_bytes(recv_sem.at[way, turn, 1], chunk * line)

                    @pl.when(turn + 1 < long)
                    def _():
                        @pl.when(step == 0)
                        def _():
                            send_mark(way, turn + 1).start()

                        send(way, turn + 1, step).start()

                    @pl.when(step == 0)
                    def _():
                        push_mark(way, turn).start()

                    push(way, turn, step).start()

            for tile in range(tiles // 2):
                tile_work(0, turn, step * (tiles // 2) + tile)
            return carry

        lax.fori_loop(0, 2, half_body, 0)
        store_sums(0, turn)

        @pl.when(turn > chips // 2)
        def _():
            send_sums(slot_of(0, turn))
            send_sums(slot_of(1, turn))

        @pl.when(turn == chips // 2)
        def _():
            send_sums(chips // 2)

        @pl.when(turn < long)
        def _():
            for way in (0, 1):
                wait_bytes(recv_sem.at[way, turn, SHORT], chunk * line)

                @pl.when(turn + 1 < long)
                def _():
                    send(way, turn + 1, SHORT).start()

                push(way, turn, SHORT).start()

        @pl.when((turn > 0) & (turn % 2 == 0))
        def _():
            hop = turn // 2
            wait_bytes(land_sem.at[long + hop - 1], 2 * set_rows * line)
            clear()

            def body(tile, carry):
                tile_work(1, hop, tile)
                return carry

            lax.fori_loop(0, tiles, body, 0)
            store_sums(1, hop)
            send_sums(hop)
            send_sums(chips - hop)

        return carry

    lax.fori_loop(0, long + 1, round_body, 0)

    sum_copy(0, 1 - core).start()
    inbox[0] = sums[core]

    for t in range(npts // LANES):
        newcov_ref[pl.ds(t, 1), :] = (
            jnp.max(best[pl.ds(t * LANES, LANES), :].T, axis=0, keepdims=True) * factor
        )

    wait_bytes(send_sem.at[0], 2 * 3 * long * chunk, rows)
    wait_bytes(send_sem.at[1], 2 * long)
    wait_bytes(push_sem.at[0], 2 * 3 * long * chunk + slots, rows)
    wait_bytes(push_sem.at[1], 2 * long + 2)
    others = chips * CORES - 1
    wait_bytes(sum_sem.at[0], others)
    wait_bytes(sum_sem.at[1], others)
    gain_ref[...] = jnp.sum(inbox[...], axis=0) * factor / total_points


def per_device(points, coverage, candidates, cand_count, acc_index):
    npts, width = points.shape
    slots = candidates.shape[0]
    blocks = lax.axis_size("blk")
    chips = blocks // CORES
    long = 2 * ((chips - 1) // 3)
    assert 3 * long == 2 * (chips - 1) and slots == LANES
    vmem = pl.BlockSpec(memory_space=pltpu.VMEM)
    hbm = pl.BlockSpec(memory_space=pltpu.HBM)
    dma = pltpu.SemaphoreType.DMA
    gain, cover = pl.pallas_call(
        functools.partial(kernel, chips, float(npts * blocks)),
        out_shape=(
            jax.ShapeDtypeStruct((1, slots), jnp.float32),
            jax.ShapeDtypeStruct((npts // LANES, LANES), jnp.float32),
        ),
        in_specs=[hbm] * 4,
        out_specs=(vmem, vmem),
        scratch_shapes=[
            pltpu.SMEM(acc_index.shape, jnp.int32),
            pltpu.VMEM((npts // LANES, LANES), jnp.float32),
            pltpu.VMEM((npts, width), jnp.bfloat16),
            pltpu.VMEM((blocks * slots, width), jnp.bfloat16),
            pltpu.VMEM((npts, LANES), jnp.float32),
            pltpu.VMEM((npts, LANES), jnp.float32),
            pltpu.VMEM((2 * (long + 1) * CORES, 1, slots), jnp.float32),
            pltpu.VMEM((CORES, 8, slots), jnp.float32),
            pltpu.VMEM((blocks, 1, slots), jnp.float32),
            pltpu.VMEM((blocks, 1, slots), jnp.float32),
            pltpu.VMEM((slots * 4 + 2, 1, LANES), jnp.float32),
            dma((5,)),
            dma((2,)),
            dma((2,)),
            dma((2, long, 3)),
            dma((3 * long // 2,)),
            dma((2,)),
        ],
        compiler_params=pltpu.CompilerParams(
            collective_id=0, has_side_effects=True, vmem_limit_bytes=48 * 1024 * 1024
        ),
        cost_estimate=pl.CostEstimate(
            flops=2 * npts * width * blocks * slots, bytes_accessed=npts * width * 2, transcendentals=0
        ),
    )(*(pltpu.with_memory_space_constraint(x, pltpu.HBM) for x in (acc_index, points, coverage.reshape(npts // LANES, LANES), candidates)))
    live = jnp.arange(slots, dtype=jnp.int32) < cand_count[0]
    return jnp.where(live, gain.reshape(slots), 0.0), cover.reshape(npts)


def solution(mesh):
    return jax.shard_map(
        per_device,
        mesh=mesh,
        in_specs=(
            P(GROUPS_BLK, None),
            P(GROUPS_BLK),
            P(GROUPS_BLK, None),
            P(GROUPS_BLK),
            P(GROUPS_BLK, None),
        ),
        out_specs=(P(GROUPS_BLK), P(GROUPS_BLK)),
        check_vma=False,
    )
```

```python
import functools

import jax
import jax.numpy as jnp
from jax import lax
from jax.experimental import pallas as pl
from jax.experimental.pallas import tpu as pltpu
from jax.sharding import PartitionSpec as P

GROUPS_BLK = ("groups", "blk")
CORES = 2
LANES = 128
TILE = 768
SHORT = 2
DEAD = -3.0e38


def kernel(
    chips, total_points, acc_hbm, points_hbm, cover_hbm, cands_hbm,
    gain_ref, newcov_ref,
    acc_ref, cover_ref, pts, rows, covb, best, marks, gacc, sums, inbox, ghost,
    load_sem, send_sem, push_sem, recv_sem, land_sem, sum_sem,
):
    npts, width = pts.shape
    slots = cands_hbm.shape[0]
    chip_rows = CORES * slots
    set_rows = slots // 2
    chunk = set_rows // 2
    short = (chips - 1) // 3
    long = 2 * short
    tiles = npts // TILE
    scale = jnp.sqrt(jnp.float32(width))
    factor = 1.0 / scale

    me = lax.axis_index("blk")
    z, core = me // CORES, me % CORES
    ahead = [((z + 1) % chips) * CORES + core, ((z + chips - 1) % chips) * CORES + core]
    partner = z * CORES + (1 - core)
    lane = lax.broadcasted_iota(jnp.int32, (1, LANES), 1)
    low = lane < set_rows

    own_at = rows.at[pl.ds(pl.multiple_of(core * slots, slots), slots)]
    accepted = pltpu.make_async_copy(acc_hbm, acc_ref, load_sem.at[0])
    own = pltpu.make_async_copy(cands_hbm, own_at, load_sem.at[1])
    covered = pltpu.make_async_copy(cover_hbm, cover_ref, load_sem.at[2])
    resident = pltpu.make_async_copy(points_hbm, pts, load_sem.at[3])
    for load in (accepted, own, covered, resident):
        load.start()

    barrier = pltpu.get_barrier_semaphore()
    for neighbour in (*ahead, partner):
        pl.semaphore_signal(barrier, inc=1, device_id={"blk": neighbour})

    accepted.wait()
    mark = jnp.full((1, LANES), DEAD, jnp.float32)
    for a in range(acc_ref.shape[1]):
        mark = jnp.where(lane == acc_ref[0, a], 0.0, mark)
    for way in (0, 1):
        marks[way * (long + 1) * CORES + core] = mark

    pl.semaphore_wait(barrier, 3)

    def slot_of(way, hop):
        return hop if way == 0 else (chips - hop) % chips

    def rows_at(way, hop, which, part, c):
        start = slot_of(way, hop) * chip_rows + c * slots + which * set_rows + part * chunk
        return rows.at[pl.ds(pl.multiple_of(start, chunk), chunk)]

    def mark_at(way, hop, c):
        return marks.at[(way * (long + 1) + hop) * CORES + c]

    def remote(src, dst, send, recv, device):
        return pltpu.make_async_remote_copy(
            src_ref=src, dst_ref=dst, send_sem=send, recv_sem=recv, device_id={"blk": device}
        )

    def where_of(way, turn, step):
        if step is SHORT:
            return turn // 2 + 1, 1 - way, turn % 2
        return turn + 1, way, step

    def send(way, turn, step):
        hop, which, part = where_of(way, turn, step)
        return remote(
            rows_at(way, hop - 1, which, part, core), rows_at(way, hop, which, part, core),
            send_sem.at[0], recv_sem.at[way, turn, step], ahead[way],
        )

    def send_mark(way, turn):
        return remote(
            mark_at(way, turn, core), mark_at(way, turn + 1, core),
            send_sem.at[1], recv_sem.at[way, turn, 0], ahead[way],
        )

    def landing(turn, step):
        return land_sem.at[long + turn // 2] if step is SHORT else land_sem.at[turn]

    def push(way, turn, step):
        hop, which, part = where_of(way, turn, step)
        at = rows_at(way, hop, which, part, core)
        return remote(at, at, push_sem.at[0], landing(turn, step), partner)

    def push_mark(way, turn):
        at = mark_at(way, turn + 1, core)
        return remote(at, at, push_sem.at[1], landing(turn, 0), partner)

    def wait_bytes(sem, count, ref=None):
        part = (ghost if ref is None else ref).at[pl.ds(0, count)]
        pltpu.make_async_copy(part, part, sem).wait()

    line = rows.shape[1] * 2 // (LANES * 4)
    own_push = [
        remote(own_at, own_at, push_sem.at[0], load_sem.at[4], partner),
        remote(mark_at(0, 0, core), mark_at(0, 0, core), push_sem.at[1], load_sem.at[4], partner),
        remote(mark_at(1, 0, core), mark_at(1, 0, core), push_sem.at[1], load_sem.at[4], partner),
    ]

    for way in (0, 1):
        send_mark(way, 0).start()
    own.wait()
    for step in (0, 1, SHORT):
        for way in (0, 1):
            send(way, 0, step).start()
    for copy in own_push:
        copy.start()

    covered.wait()
    for t in range(npts // LANES):
        row = cover_ref[pl.ds(t, 1), :] * scale
        col = jnp.broadcast_to(row, (LANES, LANES)).T
        covb[pl.ds(t * LANES, LANES), :] = col
        best[pl.ds(t * LANES, LANES), :] = col
    resident.wait()
    wait_bytes(load_sem.at[4], slots * line + 2)

    def tile_work(way, hop, tile):
        at = pl.ds(pl.multiple_of(tile * TILE, TILE), TILE)
        pieces = []
        for c in range(CORES):
            for which, path in ((0, way), (1, 1 - way)):
                start = slot_of(path, hop) * chip_rows + c * slots + which * set_rows
                pieces.append(rows[pl.ds(pl.multiple_of(start, set_rows), set_rows), :])
        similar = lax.dot_general(
            pts[at, :], jnp.concatenate(pieces, axis=0), (((1,), (1,)), ((), ())),
            preferred_element_type=jnp.float32,
        )
        cover = covb[at, :]
        high = best[at, :]
        for c in range(CORES):
            bias = jnp.where(low, mark_at(way, hop, c)[...], mark_at(1 - way, hop, c)[...])
            mine = similar[:, c * slots : (c + 1) * slots]
            over = jnp.maximum(mine - cover, 0.0)
            gacc[c] += jnp.sum(over.reshape(TILE // 8, 8, slots), axis=0)
            high = jnp.maximum(high, mine + bias)
        best[at, :] = high

    def clear():
        gacc[...] = jnp.zeros_like(gacc)

    def store_sums(way, hop):
        for c in range(CORES):
            value = jnp.sum(gacc[c], axis=0, keepdims=True)
            first = slot_of(way, hop) * CORES + c
            second = slot_of(1 - way, hop) * CORES + c
            sums[first] = jnp.where(low, value, sums[first])
            sums[second] = jnp.where(low, sums[second], value)

    def sum_copy(slot, owner_core):
        owner = ((z + chips - slot) % chips) * CORES + owner_core
        return remote(
            sums.at[slot * CORES + owner_core], inbox.at[slot * CORES + (core + owner_core) % CORES],
            sum_sem.at[0], sum_sem.at[1], owner,
        )

    def send_sums(slot):
        for c in range(CORES):
            sum_copy(slot, c).start()

    def round_body(turn, carry):
        @pl.when(turn > 0)
        def _():
            wait_bytes(land_sem.at[turn - 1], 2 * (set_rows * line + 1))

        clear()

        def half_body(step, carry):
            @pl.when(turn < long)
            def _():
                for way in (0, 1):

                    @pl.when(step == 0)
                    def _():
                        wait_bytes(recv_sem.at[way, turn, 0], chunk * line + 1)

                    @pl.when(step != 0)
                    def _():
                        wait_bytes(recv_sem.at[way, turn, 1], chunk * line)

                    @pl.when(turn + 1 < long)
                    def _():
                        @pl.when(step == 0)
                        def _():
                            send_mark(way, turn + 1).start()

                        send(way, turn + 1, step).start()

                    @pl.when(step == 0)
                    def _():
                        push_mark(way, turn).start()

                    push(way, turn, step).start()

            @pl.when((turn == long) & (step != 0))
            def _():
                for way in (0, 1):
                    wait_bytes(recv_sem.at[way, long - 1, SHORT], chunk * line)
                    push(way, long - 1, SHORT).start()

            for tile in range(tiles // 2):
                tile_work(0, turn, step * (tiles // 2) + tile)
            return carry

        lax.fori_loop(0, 2, half_body, 0)
        store_sums(0, turn)

        @pl.when(turn > chips // 2)
        def _():
            send_sums(slot_of(0, turn))
            send_sums(slot_of(1, turn))

        @pl.when(turn == chips // 2)
        def _():
            send_sums(chips // 2)

        @pl.when(turn + 1 < long)
        def _():
            for way in (0, 1):
                wait_bytes(recv_sem.at[way, turn, SHORT], chunk * line)
                send(way, turn + 1, SHORT).start()
                push(way, turn, SHORT).start()

        @pl.when((turn > 0) & (turn % 2 == 0))
        def _():
            hop = turn // 2
            wait_bytes(land_sem.at[long + hop - 1], 2 * set_rows * line)
            clear()

            def body(tile, carry):
                tile_work(1, hop, tile)
                return carry

            lax.fori_loop(0, tiles, body, 0)
            store_sums(1, hop)
            send_sums(hop)
            send_sums(chips - hop)

        return carry

    lax.fori_loop(0, long + 1, round_body, 0)

    sum_copy(0, 1 - core).start()
    inbox[0] = sums[core]

    def cover_body(block, carry):
        for nth in range(4):
            t = block * 4 + nth
            at = pl.ds(pl.multiple_of(t * LANES, LANES), LANES)
            newcov_ref[pl.ds(t, 1), :] = jnp.max(best[at, :].T, axis=0, keepdims=True) * factor
        return carry

    lax.fori_loop(0, npts // LANES // 4, cover_body, 0)

    wait_bytes(send_sem.at[0], 2 * 3 * long * chunk, rows)
    wait_bytes(send_sem.at[1], 2 * long)
    wait_bytes(push_sem.at[0], 2 * 3 * long * chunk + slots, rows)
    wait_bytes(push_sem.at[1], 2 * long + 2)
    others = chips * CORES - 1
    wait_bytes(sum_sem.at[0], others)
    wait_bytes(sum_sem.at[1], others)
    gain_ref[...] = jnp.sum(inbox[...], axis=0) * factor / total_points


def per_device(points, coverage, candidates, cand_count, acc_index):
    npts, width = points.shape
    slots = candidates.shape[0]
    blocks = lax.axis_size("blk")
    chips = blocks // CORES
    long = 2 * ((chips - 1) // 3)
    assert 3 * long == 2 * (chips - 1) and slots == LANES
    vmem = pl.BlockSpec(memory_space=pltpu.VMEM)
    hbm = pl.BlockSpec(memory_space=pltpu.HBM)
    dma = pltpu.SemaphoreType.DMA
    gain, cover = pl.pallas_call(
        functools.partial(kernel, chips, float(npts * blocks)),
        out_shape=(
            jax.ShapeDtypeStruct((1, slots), jnp.float32),
            jax.ShapeDtypeStruct((npts // LANES, LANES), jnp.float32),
        ),
        in_specs=[hbm] * 4,
        out_specs=(vmem, vmem),
        scratch_shapes=[
            pltpu.SMEM(acc_index.shape, jnp.int32),
            pltpu.VMEM((npts // LANES, LANES), jnp.float32),
            pltpu.VMEM((npts, width), jnp.bfloat16),
            pltpu.VMEM((blocks * slots, width), jnp.bfloat16),
            pltpu.VMEM((npts, LANES), jnp.float32),
            pltpu.VMEM((npts, LANES), jnp.float32),
            pltpu.VMEM((2 * (long + 1) * CORES, 1, slots), jnp.float32),
            pltpu.VMEM((CORES, 8, slots), jnp.float32),
            pltpu.VMEM((blocks, 1, slots), jnp.float32),
            pltpu.VMEM((blocks, 1, slots), jnp.float32),
            pltpu.VMEM((slots * 4 + 2, 1, LANES), jnp.float32),
            dma((5,)),
            dma((2,)),
            dma((2,)),
            dma((2, long, 3)),
            dma((3 * long // 2,)),
            dma((2,)),
        ],
        compiler_params=pltpu.CompilerParams(
            collective_id=0, has_side_effects=True, vmem_limit_bytes=48 * 1024 * 1024
        ),
        cost_estimate=pl.CostEstimate(
            flops=2 * npts * width * blocks * slots, bytes_accessed=npts * width * 2, transcendentals=0
        ),
    )(*(pltpu.with_memory_space_constraint(x, pltpu.HBM) for x in (acc_index, points, coverage.reshape(npts // LANES, LANES), candidates)))
    live = jnp.arange(slots, dtype=jnp.int32) < cand_count[0]
    return jnp.where(live, gain.reshape(slots), 0.0), cover.reshape(npts)


def solution(mesh):
    return jax.shard_map(
        per_device,
        mesh=mesh,
        in_specs=(
            P(GROUPS_BLK, None),
            P(GROUPS_BLK),
            P(GROUPS_BLK, None),
            P(GROUPS_BLK),
            P(GROUPS_BLK, None),
        ),
        out_specs=(P(GROUPS_BLK), P(GROUPS_BLK)),
        check_vma=False,
    )
```

```python
import functools

import jax
import jax.numpy as jnp
from jax import lax
from jax.experimental import pallas as pl
from jax.experimental.pallas import tpu as pltpu
from jax.sharding import PartitionSpec as P

GROUPS_BLK = ("groups", "blk")
CORES = 2
LANES = 128
TILE = 768
PARTS = 4
DEAD = -3.0e38


def kernel(
    chips, total_points, acc_hbm, points_hbm, cover_hbm, cands_hbm,
    gain_ref, newcov_ref,
    acc_ref, cover_ref, pts, rows, covb, best, marks, gacc, sums, inbox, ghost,
    load_sem, send_sem, push_sem, recv_sem, land_sem, sum_sem,
):
    npts, width = pts.shape
    slots = cands_hbm.shape[0]
    chip_rows = CORES * slots
    chunk = slots // PARTS
    far = chips // 2
    tiles = npts // TILE
    scale = jnp.sqrt(jnp.float32(width))
    factor = 1.0 / scale

    me = lax.axis_index("blk")
    z, core = me // CORES, me % CORES
    ahead = [((z + 1) % chips) * CORES + core, ((z + chips - 1) % chips) * CORES + core]
    partner = z * CORES + (1 - core)
    lane = lax.broadcasted_iota(jnp.int32, (1, LANES), 1)

    own_at = rows.at[pl.ds(pl.multiple_of(core * slots, slots), slots)]
    accepted = pltpu.make_async_copy(acc_hbm, acc_ref, load_sem.at[0])
    own = pltpu.make_async_copy(cands_hbm, own_at, load_sem.at[1])
    covered = pltpu.make_async_copy(cover_hbm, cover_ref, load_sem.at[2])
    resident = pltpu.make_async_copy(points_hbm, pts, load_sem.at[3])
    for load in (accepted, own, covered, resident):
        load.start()

    barrier = pltpu.get_barrier_semaphore()
    for neighbour in (*ahead, partner):
        pl.semaphore_signal(barrier, inc=1, device_id={"blk": neighbour})

    accepted.wait()
    mark = jnp.full((1, LANES), DEAD, jnp.float32)
    for a in range(acc_ref.shape[1]):
        mark = jnp.where(lane == acc_ref[0, a], 0.0, mark)
    marks[core] = mark

    pl.semaphore_wait(barrier, 3)

    def slot_of(way, hop):
        return hop if way == 0 else (chips - hop) % chips

    def rows_at(way, hop, part):
        nth = part if way == 0 else (part + PARTS // 2) % PARTS
        start = slot_of(way, hop) * chip_rows + core * slots + nth * chunk
        return rows.at[pl.ds(pl.multiple_of(start, chunk), chunk)]

    def mark_at(way, hop, c):
        return marks.at[slot_of(way, hop) * CORES + c]

    def remote(src, dst, send, recv, device):
        return pltpu.make_async_remote_copy(
            src_ref=src, dst_ref=dst, send_sem=send, recv_sem=recv, device_id={"blk": device}
        )

    def send(way, turn, part):
        return remote(
            rows_at(way, turn, part), rows_at(way, turn + 1, part),
            send_sem.at[0], recv_sem.at[way, turn, part], ahead[way],
        )

    def send_mark(way, turn):
        return remote(
            mark_at(way, turn, core), mark_at(way, turn + 1, core),
            send_sem.at[1], recv_sem.at[way, turn, 0], ahead[way],
        )

    def push(way, turn, part):
        at = rows_at(way, turn + 1, part)
        return remote(at, at, push_sem.at[0], land_sem.at[turn], partner)

    def push_mark(way, turn):
        at = mark_at(way, turn + 1, core)
        return remote(at, at, push_sem.at[1], land_sem.at[turn], partner)

    def wait_bytes(sem, count, ref=None):
        part = (ghost if ref is None else ref).at[pl.ds(0, count)]
        pltpu.make_async_copy(part, part, sem).wait()

    line = rows.shape[1] * 2 // (LANES * 4)
    own_push = [
        remote(own_at, own_at, push_sem.at[0], load_sem.at[4], partner),
        remote(mark_at(0, 0, core), mark_at(0, 0, core), push_sem.at[1], load_sem.at[4], partner),
    ]

    for way in (0, 1):
        send_mark(way, 0).start()
    own.wait()
    for part in range(PARTS):
        for way in (0, 1):
            send(way, 0, part).start()
    for copy in own_push:
        copy.start()

    covered.wait()
    for t in range(npts // LANES):
        row = cover_ref[pl.ds(t, 1), :] * scale
        col = jnp.broadcast_to(row, (LANES, LANES)).T
        covb[pl.ds(t * LANES, LANES), :] = col
        best[pl.ds(t * LANES, LANES), :] = col
    resident.wait()
    wait_bytes(load_sem.at[4], slots * line + 1)

    def tile_work(slot, tile):
        at = pl.ds(pl.multiple_of(tile * TILE, TILE), TILE)
        block = rows[pl.ds(pl.multiple_of(slot * chip_rows, chip_rows), chip_rows), :]
        similar = lax.dot_general(
            pts[at, :], block, (((1,), (1,)), ((), ())), preferred_element_type=jnp.float32
        )
        cover = covb[at, :]
        high = best[at, :]
        for c in range(CORES):
            mine = similar[:, c * slots : (c + 1) * slots]
            over = jnp.maximum(mine - cover, 0.0)
            gacc[c] += jnp.sum(over.reshape(TILE // 8, 8, slots), axis=0)
            high = jnp.maximum(high, mine + marks[slot * CORES + c])
        best[at, :] = high

    def sum_copy(slot, owner_core):
        owner = ((z + chips - slot) % chips) * CORES + owner_core
        return remote(
            sums.at[slot * CORES + owner_core], inbox.at[slot * CORES + (core + owner_core) % CORES],
            sum_sem.at[0], sum_sem.at[1], owner,
        )

    def send_sums(slot):
        for c in range(CORES):
            sum_copy(slot, c).start()

    def arrive(turn, part):
        for way in (0, 1):

            @pl.when((part == 0) & (turn < far - way))
            def _():
                wait_bytes(recv_sem.at[way, turn, 0], chunk * line + 1)

            @pl.when((part != 0) | (turn == far - way))
            def _():
                wait_bytes(recv_sem.at[way, turn, part], chunk * line)

            @pl.when((part == 0) & (turn + 1 < far - way))
            def _():
                send_mark(way, turn + 1).start()

            @pl.when((turn + 2 < far) | ((turn + 2 == far) & (part < PARTS // 2)))
            def _():
                send(way, turn + 1, part).start()

            @pl.when((part == 0) & (turn < far - way))
            def _():
                push_mark(way, turn).start()

            push(way, turn, part).start()

    def round_body(turn, carry):
        @pl.when((turn > 0) & (turn < far))
        def _():
            wait_bytes(land_sem.at[turn - 1], 2 * (slots * line + 1))

        @pl.when(turn == far)
        def _():
            wait_bytes(land_sem.at[turn - 1], slots * line + 1)

        def step_body(step, carry):
            way, tile = step // 2, step % 2
            slot = jnp.where(way == 0, turn, chips - turn)

            @pl.when(turn < far - 1)
            def _():
                arrive(turn, step)

            @pl.when((way == 0) | ((turn > 0) & (turn < far)))
            def _():
                @pl.when(tile == 0)
                def _():
                    gacc[...] = jnp.zeros_like(gacc)

                tile_work(slot, tile)

            @pl.when((turn == far - 1) & (tile == 0))
            def _():
                arrive(turn, way)

            @pl.when((tile == 1) & ((way == 0) | ((turn > 0) & (turn < far))))
            def _():
                for c in range(CORES):
                    sums[slot * CORES + c] = jnp.sum(gacc[c], axis=0, keepdims=True)

                @pl.when(turn > 0)
                def _():
                    send_sums(slot)

            return carry

        lax.fori_loop(0, jnp.where(turn == far, 2, PARTS), step_body, 0)
        return carry

    lax.fori_loop(0, far + 1, round_body, 0)

    sum_copy(0, 1 - core).start()
    inbox[0] = sums[core]

    for t in range(npts // LANES):
        newcov_ref[pl.ds(t, 1), :] = (
            jnp.max(best[pl.ds(t * LANES, LANES), :].T, axis=0, keepdims=True) * factor
        )

    moved = (chips - 1) * slots
    wait_bytes(send_sem.at[0], moved, rows)
    wait_bytes(send_sem.at[1], chips - 1)
    wait_bytes(push_sem.at[0], moved + slots, rows)
    wait_bytes(push_sem.at[1], chips)
    others = chips * CORES - 1
    wait_bytes(sum_sem.at[0], others)
    wait_bytes(sum_sem.at[1], others)
    gain_ref[...] = jnp.sum(inbox[...], axis=0) * factor / total_points


def per_device(points, coverage, candidates, cand_count, acc_index):
    npts, width = points.shape
    slots = candidates.shape[0]
    blocks = lax.axis_size("blk")
    chips = blocks // CORES
    far = chips // 2
    assert npts == 2 * TILE and slots == LANES
    vmem = pl.BlockSpec(memory_space=pltpu.VMEM)
    hbm = pl.BlockSpec(memory_space=pltpu.HBM)
    dma = pltpu.SemaphoreType.DMA
    gain, cover = pl.pallas_call(
        functools.partial(kernel, chips, float(npts * blocks)),
        out_shape=(
            jax.ShapeDtypeStruct((1, slots), jnp.float32),
            jax.ShapeDtypeStruct((npts // LANES, LANES), jnp.float32),
        ),
        in_specs=[hbm] * 4,
        out_specs=(vmem, vmem),
        scratch_shapes=[
            pltpu.SMEM(acc_index.shape, jnp.int32),
            pltpu.VMEM((npts // LANES, LANES), jnp.float32),
            pltpu.VMEM((npts, width), jnp.bfloat16),
            pltpu.VMEM((blocks * slots, width), jnp.bfloat16),
            pltpu.VMEM((npts, LANES), jnp.float32),
            pltpu.VMEM((npts, LANES), jnp.float32),
            pltpu.VMEM((blocks, 1, slots), jnp.float32),
            pltpu.VMEM((CORES, 8, slots), jnp.float32),
            pltpu.VMEM((blocks, 1, slots), jnp.float32),
            pltpu.VMEM((blocks, 1, slots), jnp.float32),
            pltpu.VMEM((slots * 8 + 2, 1, LANES), jnp.float32),
            dma((5,)),
            dma((2,)),
            dma((2,)),
            dma((2, far, PARTS)),
            dma((far,)),
            dma((2,)),
        ],
        compiler_params=pltpu.CompilerParams(
            collective_id=0, has_side_effects=True, vmem_limit_bytes=48 * 1024 * 1024
        ),
        cost_estimate=pl.CostEstimate(
            flops=2 * npts * width * blocks * slots, bytes_accessed=npts * width * 2, transcendentals=0
        ),
    )(*(pltpu.with_memory_space_constraint(x, pltpu.HBM) for x in (acc_index, points, coverage.reshape(npts // LANES, LANES), candidates)))
    live = jnp.arange(slots, dtype=jnp.int32) < cand_count[0]
    return jnp.where(live, gain.reshape(slots), 0.0), cover.reshape(npts)


def solution(mesh):
    return jax.shard_map(
        per_device,
        mesh=mesh,
        in_specs=(
            P(GROUPS_BLK, None),
            P(GROUPS_BLK),
            P(GROUPS_BLK, None),
            P(GROUPS_BLK),
            P(GROUPS_BLK, None),
        ),
        out_specs=(P(GROUPS_BLK), P(GROUPS_BLK)),
        check_vma=False,
    )
```

```python
import functools

import jax
import jax.numpy as jnp
from jax import lax
from jax.experimental import pallas as pl
from jax.experimental.pallas import tpu as pltpu
from jax.sharding import PartitionSpec as P

GROUPS_BLK = ("groups", "blk")
CORES = 2
LANES = 128
TILE = 768
SHORT = 2
DEAD = -3.0e38


def kernel(
    chips, total_points, acc_hbm, points_hbm, cover_hbm, cands_hbm,
    gain_ref, newcov_ref,
    acc_ref, cover_ref, pts, rows, covb, best, marks, gacc, sums, inbox, ghost,
    load_sem, send_sem, push_sem, recv_sem, land_sem, sum_sem,
):
    npts, width = pts.shape
    slots = cands_hbm.shape[0]
    chip_rows = CORES * slots
    set_rows = slots // 2
    chunk = set_rows // 2
    short = (chips - 1) // 3
    long = 2 * short
    tiles = npts // TILE
    scale = jnp.sqrt(jnp.float32(width))
    factor = 1.0 / scale

    me = lax.axis_index("blk")
    z, core = me // CORES, me % CORES
    ahead = [((z + 1) % chips) * CORES + core, ((z + chips - 1) % chips) * CORES + core]
    partner = z * CORES + (1 - core)
    lane = lax.broadcasted_iota(jnp.int32, (1, LANES), 1)
    low = lane < set_rows

    own_at = rows.at[pl.ds(pl.multiple_of(core * slots, slots), slots)]
    accepted = pltpu.make_async_copy(acc_hbm, acc_ref, load_sem.at[0])
    own = pltpu.make_async_copy(cands_hbm, own_at, load_sem.at[1])
    covered = pltpu.make_async_copy(cover_hbm, cover_ref, load_sem.at[2])
    resident = pltpu.make_async_copy(points_hbm, pts, load_sem.at[3])
    for load in (accepted, own, covered, resident):
        load.start()

    barrier = pltpu.get_barrier_semaphore()
    for neighbour in (*ahead, partner):
        pl.semaphore_signal(barrier, inc=1, device_id={"blk": neighbour})

    accepted.wait()
    mark = jnp.full((1, LANES), DEAD, jnp.float32)
    for a in range(acc_ref.shape[1]):
        mark = jnp.where(lane == acc_ref[0, a], 0.0, mark)
    for way in (0, 1):
        marks[way * (long + 1) * CORES + core] = mark

    pl.semaphore_wait(barrier, 3)

    def slot_of(way, hop):
        return hop if way == 0 else (chips - hop) % chips

    def rows_at(way, hop, which, part, c):
        start = slot_of(way, hop) * chip_rows + c * slots + which * set_rows + part * chunk
        return rows.at[pl.ds(pl.multiple_of(start, chunk), chunk)]

    def mark_at(way, hop, c):
        return marks.at[(way * (long + 1) + hop) * CORES + c]

    def remote(src, dst, send, recv, device):
        return pltpu.make_async_remote_copy(
            src_ref=src, dst_ref=dst, send_sem=send, recv_sem=recv, device_id={"blk": device}
        )

    def where_of(way, turn, step):
        if step is SHORT:
            return turn // 2 + 1, 1 - way, turn % 2
        return turn + 1, way, step

    def send(way, turn, step):
        hop, which, part = where_of(way, turn, step)
        return remote(
            rows_at(way, hop - 1, which, part, core), rows_at(way, hop, which, part, core),
            send_sem.at[0], recv_sem.at[way, turn, step], ahead[way],
        )

    def send_mark(way, turn):
        return remote(
            mark_at(way, turn, core), mark_at(way, turn + 1, core),
            send_sem.at[1], recv_sem.at[way, turn, 0], ahead[way],
        )

    def landing(turn, step):
        return land_sem.at[long + turn // 2] if step is SHORT else land_sem.at[turn]

    def push(way, turn, step):
        hop, which, part = where_of(way, turn, step)
        at = rows_at(way, hop, which, part, core)
        return remote(at, at, push_sem.at[0], landing(turn, step), partner)

    def push_mark(way, turn):
        at = mark_at(way, turn + 1, core)
        return remote(at, at, push_sem.at[1], landing(turn, 0), partner)

    def wait_bytes(sem, count, ref=None):
        part = (ghost if ref is None else ref).at[pl.ds(0, count)]
        pltpu.make_async_copy(part, part, sem).wait()

    line = rows.shape[1] * 2 // (LANES * 4)
    own_push = [
        remote(own_at, own_at, push_sem.at[0], load_sem.at[4], partner),
        remote(mark_at(0, 0, core), mark_at(0, 0, core), push_sem.at[1], load_sem.at[4], partner),
        remote(mark_at(1, 0, core), mark_at(1, 0, core), push_sem.at[1], load_sem.at[4], partner),
    ]

    for way in (0, 1):
        send_mark(way, 0).start()
    own.wait()
    for step in (0, 1, SHORT):
        for way in (0, 1):
            send(way, 0, step).start()
    for copy in own_push:
        copy.start()

    covered.wait()
    for t in range(npts // LANES):
        row = cover_ref[pl.ds(t, 1), :] * scale
        col = jnp.broadcast_to(row, (LANES, LANES)).T
        covb[pl.ds(t * LANES, LANES), :] = col
        best[pl.ds(t * LANES, LANES), :] = col
    resident.wait()
    wait_bytes(load_sem.at[4], slots * line + 2)

    def tile_work(way, hop, tile):
        at = pl.ds(pl.multiple_of(tile * TILE, TILE), TILE)
        pieces = []
        for c in range(CORES):
            for which, path in ((0, way), (1, 1 - way)):
                start = slot_of(path, hop) * chip_rows + c * slots + which * set_rows
                pieces.append(rows[pl.ds(pl.multiple_of(start, set_rows), set_rows), :])
        similar = lax.dot_general(
            pts[at, :], jnp.concatenate(pieces, axis=0), (((1,), (1,)), ((), ())),
            preferred_element_type=jnp.float32,
        )
        cover = covb[at, :]
        high = best[at, :]
        for c in range(CORES):
            bias = jnp.where(low, mark_at(way, hop, c)[...], mark_at(1 - way, hop, c)[...])
            mine = similar[:, c * slots : (c + 1) * slots]
            over = jnp.maximum(mine - cover, 0.0)
            gacc[c] += jnp.sum(over.reshape(TILE // 8, 8, slots), axis=0)
            high = jnp.maximum(high, mine + bias)
        best[at, :] = high

    def clear():
        gacc[...] = jnp.zeros_like(gacc)

    def store_sums(way, hop):
        for c in range(CORES):
            value = jnp.sum(gacc[c], axis=0, keepdims=True)
            first = slot_of(way, hop) * CORES + c
            second = slot_of(1 - way, hop) * CORES + c
            sums[first] = jnp.where(low, value, sums[first])
            sums[second] = jnp.where(low, sums[second], value)

    def sum_copy(slot, owner_core):
        owner = ((z + chips - slot) % chips) * CORES + owner_core
        return remote(
            sums.at[slot * CORES + owner_core], inbox.at[slot * CORES + (core + owner_core) % CORES],
            sum_sem.at[0], sum_sem.at[1], owner,
        )

    def send_sums(slot):
        for c in range(CORES):
            sum_copy(slot, c).start()

    def round_body(turn, carry):
        @pl.when(turn > 0)
        def _():
            wait_bytes(land_sem.at[turn - 1], 2 * (set_rows * line + 1))

        clear()

        def half_body(step, carry):
            @pl.when(turn < long)
            def _():
                for way in (0, 1):

                    @pl.when(step == 0)
                    def _():
                        wait_bytes(recv_sem.at[way, turn, 0], chunk * line + 1)

                    @pl.when(step != 0)
                    def _():
                        wait_bytes(recv_sem.at[way, turn, 1], chunk * line)

                    @pl.when(turn + 1 < long)
                    def _():
                        @pl.when(step == 0)
                        def _():
                            send_mark(way, turn + 1).start()

                        send(way, turn + 1, step).start()

                    @pl.when(step == 0)
                    def _():
                        push_mark(way, turn).start()

                    push(way, turn, step).start()

            @pl.when((turn == long) & (step != 0))
            def _():
                for way in (0, 1):
                    wait_bytes(recv_sem.at[way, long - 1, SHORT], chunk * line)
                    push(way, long - 1, SHORT).start()

            for tile in range(tiles // 2):
                tile_work(0, turn, step * (tiles // 2) + tile)
            return carry

        lax.fori_loop(0, 2, half_body, 0)
        store_sums(0, turn)

        @pl.when(turn > chips // 2)
        def _():
            send_sums(slot_of(0, turn))
            send_sums(slot_of(1, turn))

        @pl.when(turn == chips // 2)
        def _():
            send_sums(chips // 2)

        @pl.when(turn + 1 < long)
        def _():
            for way in (0, 1):
                wait_bytes(recv_sem.at[way, turn, SHORT], chunk * line)
                send(way, turn + 1, SHORT).start()
                push(way, turn, SHORT).start()

        @pl.when((turn > 0) & (turn % 2 == 0))
        def _():
            hop = turn // 2
            wait_bytes(land_sem.at[long + hop - 1], 2 * set_rows * line)
            clear()

            def body(tile, carry):
                tile_work(1, hop, tile)
                return carry

            lax.fori_loop(0, tiles, body, 0)
            store_sums(1, hop)
            send_sums(hop)
            send_sums(chips - hop)

        return carry

    lax.fori_loop(0, long + 1, round_body, 0)

    sum_copy(0, 1 - core).start()
    inbox[0] = sums[core]

    def cover_body(block, carry):
        for nth in range(4):
            t = block * 4 + nth
            at = pl.ds(pl.multiple_of(t * LANES, LANES), LANES)
            newcov_ref[pl.ds(t, 1), :] = jnp.max(best[at, :].T, axis=0, keepdims=True) * factor
        return carry

    lax.fori_loop(0, npts // LANES // 4, cover_body, 0)

    wait_bytes(send_sem.at[0], 2 * 3 * long * chunk, rows)
    wait_bytes(send_sem.at[1], 2 * long)
    wait_bytes(push_sem.at[0], 2 * 3 * long * chunk + slots, rows)
    wait_bytes(push_sem.at[1], 2 * long + 2)
    others = chips * CORES - 1
    wait_bytes(sum_sem.at[0], others)
    wait_bytes(sum_sem.at[1], others)
    gain_ref[...] = jnp.sum(inbox[...], axis=0) * factor / total_points


def finish(count_ref, gain_ref, cover_ref, gain_hbm, cover_hbm, live_ref, sems):
    covered = pltpu.make_async_copy(cover_ref, cover_hbm, sems.at[0])
    covered.start()
    lane = lax.broadcasted_iota(jnp.int32, gain_ref.shape, 1)
    live_ref[...] = jnp.where(lane < count_ref[0], gain_ref[...], 0.0)
    gained = pltpu.make_async_copy(live_ref, gain_hbm, sems.at[1])
    gained.start()
    covered.wait()
    gained.wait()


def finished(count, gain, cover):
    vmem = pl.BlockSpec(memory_space=pltpu.VMEM)
    hbm = pl.BlockSpec(memory_space=pltpu.HBM)
    gain_out, cover_out = pl.pallas_call(
        finish,
        out_shape=(
            jax.ShapeDtypeStruct(gain.shape, gain.dtype),
            jax.ShapeDtypeStruct(cover.shape, cover.dtype),
        ),
        in_specs=[pl.BlockSpec(memory_space=pltpu.SMEM), vmem, vmem],
        out_specs=(hbm, hbm),
        scratch_shapes=[pltpu.VMEM(gain.shape, gain.dtype), pltpu.SemaphoreType.DMA((2,))],
        compiler_params=pltpu.CompilerParams(vmem_limit_bytes=1024 * 1024),
    )(count, gain, cover)
    return gain_out.reshape(gain.size), cover_out.reshape(cover.size)


def per_device(points, coverage, candidates, cand_count, acc_index):
    npts, width = points.shape
    slots = candidates.shape[0]
    blocks = lax.axis_size("blk")
    chips = blocks // CORES
    long = 2 * ((chips - 1) // 3)
    assert 3 * long == 2 * (chips - 1) and slots == LANES
    vmem = pl.BlockSpec(memory_space=pltpu.VMEM)
    hbm = pl.BlockSpec(memory_space=pltpu.HBM)
    dma = pltpu.SemaphoreType.DMA
    gain, cover = pl.pallas_call(
        functools.partial(kernel, chips, float(npts * blocks)),
        out_shape=(
            jax.ShapeDtypeStruct((1, slots), jnp.float32),
            jax.ShapeDtypeStruct((npts // LANES, LANES), jnp.float32),
        ),
        in_specs=[hbm] * 4,
        out_specs=(vmem, vmem),
        scratch_shapes=[
            pltpu.SMEM(acc_index.shape, jnp.int32),
            pltpu.VMEM((npts // LANES, LANES), jnp.float32),
            pltpu.VMEM((npts, width), jnp.bfloat16),
            pltpu.VMEM((blocks * slots, width), jnp.bfloat16),
            pltpu.VMEM((npts, LANES), jnp.float32),
            pltpu.VMEM((npts, LANES), jnp.float32),
            pltpu.VMEM((2 * (long + 1) * CORES, 1, slots), jnp.float32),
            pltpu.VMEM((CORES, 8, slots), jnp.float32),
            pltpu.VMEM((blocks, 1, slots), jnp.float32),
            pltpu.VMEM((blocks, 1, slots), jnp.float32),
            pltpu.VMEM((slots * 4 + 2, 1, LANES), jnp.float32),
            dma((5,)),
            dma((2,)),
            dma((2,)),
            dma((2, long, 3)),
            dma((3 * long // 2,)),
            dma((2,)),
        ],
        compiler_params=pltpu.CompilerParams(
            collective_id=0, has_side_effects=True, vmem_limit_bytes=48 * 1024 * 1024
        ),
        cost_estimate=pl.CostEstimate(
            flops=2 * npts * width * blocks * slots, bytes_accessed=npts * width * 2, transcendentals=0
        ),
    )(*(pltpu.with_memory_space_constraint(x, pltpu.HBM) for x in (acc_index, points, coverage.reshape(npts // LANES, LANES), candidates)))
    return finished(cand_count, gain, cover)


def solution(mesh):
    return jax.shard_map(
        per_device,
        mesh=mesh,
        in_specs=(
            P(GROUPS_BLK, None),
            P(GROUPS_BLK),
            P(GROUPS_BLK, None),
            P(GROUPS_BLK),
            P(GROUPS_BLK, None),
        ),
        out_specs=(P(GROUPS_BLK), P(GROUPS_BLK)),
        check_vma=False,
    )
```
